32 devices in a mesh: fsdp: 8 (over z, core), head: 4 (over y, x).
Axes of the slice: x: 2, y: 2, z: 4, core: 2. Of those that a mesh axis runs over, the one named last changes fastest.
Arguments:
- probe_compressed: bfloat16 [2, 32, 1536], P(None, 'fsdp'), may hold values from -6 to 6
- w_uq: bfloat16 [1536, 16384], P('fsdp', 'head'), may hold values from -0.15625 to 0.15625
- w_qr: bfloat16 [1536, 8192], P('fsdp', 'head'), may hold values from -0.15625 to 0.15625
- w_uk: bfloat16 [512, 16384], P('fsdp', 'head'), may hold values from -0.25 to 0.25
- w_uv: bfloat16 [512, 16384], P('fsdp', 'head'), may hold values from -1.5 to 1.5
- cache: bfloat16 [32, 1024, 576], P(('fsdp', 'head')), may hold values from -136 to 136
- new_kv: bfloat16 [2, 32, 576], P(None, ('fsdp', 'head')), may hold values from -6 to 6
- lengths: int32 [32], P(('fsdp', 'head')), may hold values from 1 to 1024
Outputs:
- values: bfloat16 [2, 32, 16384], P(None, 'fsdp', 'head')
The draws below stay inside these ranges and needn't reach their ends.
All inputs are finite; a program needn't handle non-finite values.
Results may differ from the reference program's by a relative error of at most 0.035.
Values may be sent and summed in bfloat16 or wider, within the bound.
A program may use at most 64 MiB of HBM per device.

```python
import jax
import jax.numpy as jnp
from jax import lax

H = 128
QR = 1536
C = 512
NOPE = 128
R = 64
VDIM = 128
STORED_POSITIONS = 1024
STEPS = 2
SEQUENCE_COUNT = 32


def draw_cache(key, part):
    shape = (SEQUENCE_COUNT, STORED_POSITIONS, C + R)
    values = jnp.clip(jax.random.normal(jax.random.fold_in(key, 11), shape, jnp.float32), -6.0, 6.0)
    return values.astype(jnp.bfloat16)


def with_ends(entries, own_key, low, largest):
    place = [jax.random.randint(jax.random.fold_in(own_key, axis), (), 0, length) for axis, length in enumerate(entries.shape)]
    widest = entries.shape.index(max(entries.shape))
    neighbour = place[:widest] + [(place[widest] + 1) % entries.shape[widest]] + place[widest + 1:]
    return entries.at[tuple(place)].set(low).at[tuple(neighbour)].set(largest)


def steps_of(key, dims, cuts, smallest, largest):
    loudness, own = 1.0, jax.random.fold_in(key, 6)
    for axis_at, parts in cuts:
        steps = jnp.exp(jax.random.uniform(jax.random.fold_in(own, axis_at), (parts,), jnp.float32, smallest / len(cuts), largest / len(cuts)))
        loudness = loudness * jnp.repeat(steps, dims[axis_at] // parts).reshape([-1 if axis == axis_at else 1 for axis in range(len(dims))])
    return loudness


def scatter_about(rng, dims, deviation, most, cuts=(), kind=jnp.bfloat16):
    array = deviation * jax.random.normal(rng, dims, jnp.float32)
    if cuts:
        array = array * steps_of(rng, dims, cuts, -0.22, 0.18)
    return jnp.clip(array, -most, most).astype(kind)


def setup_inputs(seed: int = 0) -> dict:
    key_of = jax.random.split(jax.random.key(seed), 9)
    probe_compressed = scatter_about(key_of[0], (STEPS, SEQUENCE_COUNT, QR), 1.0, 6.0, ((1, 8),))
    w_uq = scatter_about(key_of[1], (QR, H * NOPE), QR ** -0.5, 0.15625, ((0, 8), (1, 4)))
    w_qr = scatter_about(key_of[2], (QR, H * R), QR ** -0.5, 0.15625, ((0, 8), (1, 4)))
    w_uk = scatter_about(key_of[3], (C, H * NOPE), C ** -0.5, 0.25, ((0, 8), (1, 4)))
    w_uv = scatter_about(key_of[4], (C, H * VDIM), 0.25, 1.5, ((0, 8), (1, 4)))
    cache = draw_cache(jax.random.fold_in(key_of[8], 71), 0)
    new_kv = scatter_about(key_of[6], (STEPS, SEQUENCE_COUNT, C + R), 1.0, 6.0, ((1, 32),))
    lengths = with_ends(jax.random.randint(key_of[7], (SEQUENCE_COUNT,), 1, STORED_POSITIONS + 1), jax.random.fold_in(key_of[7], 1), 1, STORED_POSITIONS).astype(jnp.int32)
    return {"probe_compressed": probe_compressed, "w_uq": w_uq, "w_qr": w_qr, "w_uk": w_uk, "w_uv": w_uv, "cache": cache, "new_kv": new_kv, "lengths": lengths}


def rotate(rope_part, position):
    half = rope_part.shape[-1] // 2
    freqs = 10000.0 ** (-(jnp.arange(half, dtype=jnp.float32) * 2.0 / (2 * half)))
    angle = position[..., None] * freqs
    first = rope_part[..., :half]
    second = rope_part[..., half:]
    cosine_table = jnp.cos(angle)
    sine = jnp.sin(angle)
    return jnp.concatenate([first * cosine_table - second * sine, first * sine + second * cosine_table], axis=-1)


def attend(query, keys, fresh, extent):
    steps = query.shape[0]
    heads = query.shape[1]
    width = keys.shape[1]
    latent_width = width - R
    position = (extent + jnp.arange(steps, dtype=jnp.int32)).astype(jnp.float32)
    rotated = rotate(query[:, :, latent_width:].astype(jnp.float32), position[:, None])
    joined = jnp.concatenate([query[:, :, :latent_width], rotated.astype(jnp.bfloat16)], axis=2)
    joined = joined.reshape(steps * heads, width)
    factor = (NOPE + R) ** -0.5
    older = jnp.dot(joined, keys.T, preferred_element_type=jnp.float32) * factor
    valid = jnp.arange(keys.shape[0], dtype=jnp.int32) < extent
    older = jnp.where(valid[None, :], older, -1e30)
    newer = jnp.dot(joined, fresh.T, preferred_element_type=jnp.float32) * factor
    order = jnp.arange(steps, dtype=jnp.int32)
    allowed = jnp.repeat(order[None, :] <= order[:, None], heads, axis=0)
    newer = jnp.where(allowed, newer, -1e30)
    highest = jnp.maximum(jnp.max(older, axis=1), jnp.max(newer, axis=1))
    weight_old = jnp.exp(older - highest[:, None])
    weight_new = jnp.exp(newer - highest[:, None])
    total = jnp.sum(weight_old, axis=1) + jnp.sum(weight_new, axis=1)
    mixed = jnp.dot(weight_old.astype(jnp.bfloat16), keys[:, :latent_width], preferred_element_type=jnp.float32)
    mixed = mixed + jnp.dot(weight_new.astype(jnp.bfloat16), fresh[:, :latent_width], preferred_element_type=jnp.float32)
    return (mixed / total[:, None]).astype(jnp.bfloat16).reshape(steps, heads, latent_width)


def reference(probe_compressed, w_uq, w_qr, w_uk, w_uv, cache, new_kv, lengths):
    flattened = probe_compressed.reshape(STEPS * SEQUENCE_COUNT, QR)
    query_heads = w_uq.reshape(QR, H, NOPE).transpose(1, 0, 2)
    rope_heads = w_qr.reshape(QR, H, R).transpose(1, 0, 2)
    key_heads = w_uk.reshape(C, H, NOPE).transpose(1, 0, 2)

    def head_query(pieces):
        query_up, rotary_up_weight, key_up = pieces
        absorbed = jnp.dot(query_up, key_up.T, preferred_element_type=jnp.float32).astype(jnp.bfloat16)
        latent = jnp.dot(flattened, absorbed, preferred_element_type=jnp.float32).astype(jnp.bfloat16)
        rope_query = jnp.dot(flattened, rotary_up_weight, preferred_element_type=jnp.float32).astype(jnp.bfloat16)
        return jnp.concatenate([latent, rope_query], axis=1)

    query_matrix = lax.map(head_query, (query_heads, rope_heads, key_heads))
    query_matrix = query_matrix.reshape(H, STEPS, SEQUENCE_COUNT, C + R).transpose(2, 1, 0, 3)
    value_up = w_uv.reshape(C, H, VDIM).astype(jnp.float32)

    def row_attend(pieces):
        query, keys, fresh, extent = pieces
        mixed = attend(query, keys, fresh, extent)
        attention_output = jnp.einsum("shc,chv->shv", mixed.astype(jnp.float32), value_up)
        return attention_output.astype(jnp.bfloat16).reshape(STEPS, H * VDIM)

    values = lax.map(row_attend, (query_matrix, cache, new_kv.transpose(1, 0, 2), lengths))
    return values.transpose(1, 0, 2)
```

```python
import functools

import jax
import jax.numpy as jnp
import numpy as np
from jax import lax
from jax.experimental import pallas as pl
from jax.experimental.pallas import tpu as pltpu
from jax.sharding import PartitionSpec as P

NOPE = 128
R = 64
VDIM = 128


def rotate(rope_part, position):
    half = rope_part.shape[-1] // 2
    freqs = 10000.0 ** (-(jnp.arange(half, dtype=jnp.float32) * 2.0 / (2 * half)))
    angle = position[..., None] * freqs
    first = rope_part[..., :half]
    second = rope_part[..., half:]
    cosine_table = jnp.cos(angle)
    sine = jnp.sin(angle)
    return jnp.concatenate(
        [first * cosine_table - second * sine, first * sine + second * cosine_table], axis=-1
    )


def attend(query, keys, fresh, extent):
    steps = query.shape[0]
    heads = query.shape[1]
    width = keys.shape[1]
    latent_width = width - R
    position = (extent + jnp.arange(steps, dtype=jnp.int32)).astype(jnp.float32)
    rotated = rotate(query[:, :, latent_width:].astype(jnp.float32), position[:, None])
    joined = jnp.concatenate([query[:, :, :latent_width], rotated.astype(jnp.bfloat16)], axis=2)
    joined = joined.reshape(steps * heads, width)
    factor = (NOPE + R) ** (-0.5)
    older = jnp.dot(joined, keys.T, preferred_element_type=jnp.float32) * factor
    valid = jnp.arange(keys.shape[0], dtype=jnp.int32) < extent
    older = jnp.where(valid[None, :], older, -1e30)
    newer = jnp.dot(joined, fresh.T, preferred_element_type=jnp.float32) * factor
    order = jnp.arange(steps, dtype=jnp.int32)
    allowed = jnp.repeat(order[None, :] <= order[:, None], heads, axis=0)
    newer = jnp.where(allowed, newer, -1e30)
    highest = jnp.maximum(jnp.max(older, axis=1), jnp.max(newer, axis=1))
    weight_old = jnp.exp(older - highest[:, None])
    weight_new = jnp.exp(newer - highest[:, None])
    total = jnp.sum(weight_old, axis=1) + jnp.sum(weight_new, axis=1)
    mixed = jnp.dot(
        weight_old.astype(jnp.bfloat16), keys[:, :latent_width], preferred_element_type=jnp.float32
    )
    mixed = mixed + jnp.dot(
        weight_new.astype(jnp.bfloat16), fresh[:, :latent_width], preferred_element_type=jnp.float32
    )
    return (mixed / total[:, None]).astype(jnp.bfloat16).reshape(steps, heads, latent_width)


def per_device(probe_compressed, w_uq, w_qr, w_uk, w_uv, cache, new_kv, lengths):
    heads = w_uk.shape[1] // NOPE
    steps, group, rank = probe_compressed.shape
    flattened = probe_compressed.reshape(steps * group, rank)
    key_up, value_up, rotary_up_weight = (
        lax.all_gather(w_uk, "fsdp", axis=0, tiled=True),
        lax.all_gather(w_uv, "fsdp", axis=0, tiled=True),
        lax.all_gather(w_qr, "fsdp", axis=0, tiled=True),
    )
    key_heads = key_up.reshape(key_up.shape[0], heads, NOPE)
    slab = lax.all_gather(w_uq, "fsdp", axis=0, tiled=True)
    count = slab.shape[0]
    slab_heads = slab.reshape(count, heads, NOPE)
    absorbed = jnp.einsum("rhn,chn->hrc", slab_heads, key_heads, preferred_element_type=jnp.float32)
    absorbed = absorbed.astype(jnp.bfloat16)
    summed = jnp.einsum("qr,hrc->qhc", flattened, absorbed, preferred_element_type=jnp.float32)
    latent = summed.astype(jnp.bfloat16)
    latent_rank = key_up.shape[0]
    rope_query = jnp.dot(flattened, rotary_up_weight, preferred_element_type=jnp.float32).astype(
        jnp.bfloat16
    )
    rope_query = rope_query.reshape(steps * group, heads, R)
    query_matrix = jnp.concatenate([latent, rope_query], axis=2).reshape(
        steps, group, heads, latent_rank + R
    )
    row_queries = lax.all_to_all(query_matrix, "head", split_axis=1, concat_axis=2, tiled=True)
    mixed = jax.vmap(attend, in_axes=(1, 0, 1, 0), out_axes=1)(row_queries, cache, new_kv, lengths)
    combined_across_heads = lax.all_to_all(mixed, "head", split_axis=2, concat_axis=1, tiled=True)
    value_heads = value_up.reshape(latent_rank, heads, VDIM)
    attention_output = jnp.einsum(
        "sghc,chv->sghv", combined_across_heads, value_heads, preferred_element_type=jnp.float32
    )
    return attention_output.astype(jnp.bfloat16).reshape(steps, group, heads * VDIM)


def fused(F, G, steps, own,
          len_ref, freq_ref, probe_ref, new_ref, uq_hbm, qr_hbm, uk_hbm, uv_hbm, cache_hbm,
          out_ref,
          uq, wqr, wk, wv, kv, ps, pr, pp, pv, zs, zr, qs, qr, ms, mr, os_, or_,
          lsem, sp, rp, sk, rk, sv, rv, spp, rpp, sz, rz, sq, rq, sm, rm, so, ro):
    f32, bf16 = jnp.float32, jnp.bfloat16
    f = lax.axis_index("fsdp")
    hd = lax.axis_index("head")
    N = F * G
    Z = F // 2
    me = f * G + hd
    z, core = lax.div(f, 2), lax.rem(f, 2)
    ck = uk_hbm.shape[0]
    cols = own * NOPE
    rcols = own * R
    C = ck * F
    stored = cache_hbm.shape[1]
    slice_rank = uq.shape[0]
    per = steps * own
    queries = F * steps * G
    expanded = N * per

    def rcopy(src, dst, ssem, rsem, ff, hh):
        return pltpu.make_async_remote_copy(
            src_ref=src, dst_ref=dst, send_sem=ssem, recv_sem=rsem,
            device_id={"fsdp": ff, "head": hh}, device_id_type=pl.DeviceIdType.MESH,
        )

    def block(t, width):
        return pl.ds(pl.multiple_of(t * width, 128), width)

    mine = pl.ds(pl.multiple_of(f * ck, 16), ck)
    load_uq = pltpu.make_async_copy(uq_hbm, uq, lsem.at[0])
    load_qr = pltpu.make_async_copy(qr_hbm, wqr, lsem.at[1])
    load_kv = pltpu.make_async_copy(cache_hbm.at[0], kv.at[pl.ds(0, stored)], lsem.at[2])
    load_uk = pltpu.make_async_copy(uk_hbm.at[:, block(f, cols)], wk.at[mine], lsem.at[3])
    load_uv = pltpu.make_async_copy(uv_hbm.at[:, block(f, cols)], wv.at[mine], lsem.at[4])
    loads = [load_uq, load_qr, load_kv, load_uk, load_uv]
    for c in loads:
        c.start()

    bar = pltpu.get_barrier_semaphore()

    def greet(k, carry):
        t = lax.rem(me + k, N)
        pl.semaphore_signal(
            bar, inc=1, device_id={"fsdp": lax.div(t, G), "head": lax.rem(t, G)},
            device_id_type=pl.DeviceIdType.MESH,
        )
        return carry

    lax.fori_loop(1, N, greet, 0)

    probe8 = jnp.concatenate([probe_ref[s].astype(f32) for s in range(steps)], axis=0)
    for p in range(F):
        ps[p] = probe8[:, p * slice_rank:(p + 1) * slice_rank].astype(bf16)
    pr[pl.ds(f, 1)] = ps[pl.ds(f, 1)]

    pl.semaphore_wait(bar, N - 1)

    def probe_copy(k):
        t = lax.rem(f + k, F)
        return rcopy(ps.at[t], pr.at[f], sp.at[k], rp.at[f], t, hd)

    def uk_copy(k):
        t = lax.rem(f + k, F)
        return rcopy(uk_hbm.at[:, block(t, cols)], wk.at[mine], sk.at[k], rk.at[f], t, hd)

    def uv_copy(k):
        t = lax.rem(f + k, F)
        return rcopy(uv_hbm.at[:, block(t, cols)], wv.at[mine], sv.at[k], rv.at[f], t, hd)

    def each(first, last, make, method):
        def step(k, carry):
            getattr(make(k), method)()
            return carry
        lax.fori_loop(first, last, step, 0)

    each(1, F, probe_copy, "start")
    each(1, F, uk_copy, "start")

    tail = kv.shape[0] - stored
    at = lax.broadcasted_iota(jnp.int32, (tail, kv.shape[1]), 0)
    fill = jnp.zeros((tail, kv.shape[1]), f32)
    for s in range(steps):
        fill = jnp.where(at == s, new_ref[s].astype(f32), fill)
    kv[stored:stored + tail, :] = fill.astype(bf16)

    row8 = lax.broadcasted_iota(jnp.int32, (per, 128), 0)
    step8 = lax.div(row8, own)
    angle = (len_ref[0] + step8).astype(f32) * freq_ref[...]
    cos8, sin8 = jnp.cos(angle), jnp.sin(angle)

    load_uq.wait()
    load_qr.wait()

    def probe_arrival(k, carry):
        src = lax.rem(f + k, F)
        rcopy(ps.at[src], pr.at[src], sp.at[k], rp.at[src], src, hd).wait_recv()
        return carry

    lax.fori_loop(1, F, probe_arrival, 0)
    probes = pr[...].astype(f32).reshape(queries, slice_rank).astype(bf16)

    def partial_of(t):
        a = jnp.dot(probes, uq[:, block(t, cols)], preferred_element_type=f32)
        b = jnp.dot(probes, wqr[:, block(t, rcols)], preferred_element_type=f32)
        return a, b

    def pair_copy(k):
        zz = lax.rem(z + k, Z)
        return rcopy(pp.at[zz], pv.at[zz], spp.at[zz], rpp.at[zz], z * 2 + 1 - core, hd)

    def to_partner(k, carry):
        zz = lax.rem(z + k, Z)
        a, b = partial_of(zz * 2 + 1 - core)
        pp[zz, :, 0:cols] = a.astype(bf16)
        pp[zz, :, cols:cols + rcols] = b.astype(bf16)
        pair_copy(k).start()
        return carry

    lax.fori_loop(1, Z + 1, to_partner, 0)

    def line_copy(k):
        zz = lax.rem(z + k, Z)
        return rcopy(zs.at[zz], zr.at[z], sz.at[zz], rz.at[z], zz * 2 + core, hd)

    def along_line(k, carry):
        zz = lax.rem(z + k, Z)
        a, b = partial_of(zz * 2 + core)
        pair_copy(k).wait_recv()
        zs[zz, :, 0:cols] = (a + pv[zz, :, 0:cols].astype(f32)).astype(bf16)
        zs[zz, :, cols:cols + rcols] = (b + pv[zz, :, cols:cols + rcols].astype(f32)).astype(bf16)
        line_copy(k).start()
        return carry

    lax.fori_loop(1, Z, along_line, 0)
    a, b = partial_of(f)
    pair_copy(0).wait_recv()
    nope = a + pv[z, :, 0:cols].astype(f32)
    rope = b + pv[z, :, cols:cols + rcols].astype(f32)
    for k in range(1, Z):
        src = lax.rem(z + k, Z)
        rcopy(zs.at[src], zr.at[src], sz.at[src], rz.at[src], src * 2 + core, hd).wait_recv()
        nope = nope + zr[src, :, 0:cols].astype(f32)
        rope = rope + zr[src, :, cols:cols + rcols].astype(f32)
    nope = nope.astype(bf16)
    rope = rope.astype(bf16)

    def iota(shape, axis):
        return lax.broadcasted_iota(jnp.int32, shape, axis)

    er = iota((expanded, queries), 0)
    ed = lax.div(er, per)
    es = lax.div(lax.rem(er, per), own)
    pick = (lax.div(ed, G) * (steps * G) + es * G + lax.rem(ed, G)) == iota((expanded, queries), 1)
    pick = jnp.where(pick, 1.0, 0.0).astype(bf16)
    head_of_row = lax.rem(iota((expanded, cols), 0), own)
    own_head = lax.div(iota((expanded, cols), 1), NOPE) == head_of_row
    own_rope = lax.div(iota((expanded, rcols), 1), R) == lax.rem(iota((expanded, rcols), 0), own)
    fold = lax.rem(iota((rcols, 128), 0), R) == iota((rcols, 128), 1)
    fold = jnp.where(fold, 1.0, 0.0).astype(bf16)
    wide = jnp.where(own_head, jnp.dot(pick, nope, preferred_element_type=f32), 0.0).astype(bf16)
    wide_rope = jnp.where(own_rope, jnp.dot(pick, rope, preferred_element_type=f32), 0.0).astype(bf16)
    rope_rows = jnp.dot(wide_rope, fold, preferred_element_type=f32)

    load_uk.wait()

    def weight_arrival(hbm, w, ssem, rsem):
        def step(k, carry):
            src = lax.rem(f + k, F)
            there = pl.ds(pl.multiple_of(src * ck, 16), ck)
            rcopy(hbm.at[:, block(src, cols)], w.at[there], ssem.at[k], rsem.at[src], src, hd).wait_recv()
            return carry
        lax.fori_loop(1, F, step, 0)

    weight_arrival(uk_hbm, wk, sk, rk)
    latent = lax.dot_general(wide, wk[...], (((1,), (1,)), ((), ())), preferred_element_type=f32)
    qs[:, :, 0:C] = latent.reshape(N, per, C).astype(bf16)
    qs[:, :, C:C + 128] = rope_rows.reshape(N, per, 128).astype(bf16)

    def query_copy(k):
        t = lax.rem(me + k, N)
        return rcopy(qs.at[t], qr.at[me], sq.at[k], rq.at[me], lax.div(t, G), lax.rem(t, G))

    each(1, N, query_copy, "start")
    each(1, F, uv_copy, "start")
    qr[pl.ds(me, 1)] = qs[pl.ds(me, 1)]

    load_kv.wait()
    factor = (NOPE + R) ** -0.5
    chunk = F
    sr = iota((128, 128), 0)
    sc = iota((128, 128), 1)
    half = R // 2
    swap = jnp.where((sr == sc + half) & (sc < half), -1.0, 0.0)
    swap = swap + jnp.where((sr == sc - half) & (sc >= half) & (sc < R), 1.0, 0.0)
    swap = swap.astype(bf16)
    rows = chunk * per
    keys = kv.shape[0]
    cosines = jnp.broadcast_to(cos8[None], (chunk, per, 128)).reshape(rows, 128)
    sines = jnp.broadcast_to(sin8[None], (chunk, per, 128)).reshape(rows, 128)
    column = iota((rows, keys), 1)
    step_of = lax.div(lax.rem(iota((rows, keys), 0), per), own)
    shown = (column < len_ref[0]) | ((column >= stored) & (column <= stored + step_of))

    def mixed_copy(e):
        return rcopy(ms.at[e], mr.at[me], sm.at[e], rm.at[me], lax.div(e, G), lax.rem(e, G))

    def attend_chunk(b, carry):
        base = b * chunk

        def arrival(i, c):
            src = base + i

            @pl.when(src != me)
            def _():
                rcopy(qs.at[src], qr.at[src], sq.at[0], rq.at[src], lax.div(src, G), lax.rem(src, G)).wait_recv()
            return c

        lax.fori_loop(0, chunk, arrival, 0)
        x = qr[pl.ds(base, chunk)].astype(f32).reshape(rows, C + 128)
        lat = x[:, 0:C].astype(bf16)
        xr = x[:, C:C + 128]
        turned = jnp.dot(xr.astype(bf16), swap, preferred_element_type=f32)
        rot = (xr * cosines + turned * sines).astype(bf16)[:, 0:R]
        nt = (((1,), (1,)), ((), ()))
        s = lax.dot_general(lat, kv[:, 0:C], nt, preferred_element_type=f32)
        s = s + lax.dot_general(rot, kv[:, C:C + R], nt, preferred_element_type=f32)
        s = jnp.where(shown, s * factor, -1e30)
        m = jnp.max(s, axis=1, keepdims=True)
        w = jnp.exp(s - m)
        total = jnp.sum(w, axis=1, keepdims=True)
        mix = jnp.dot(w.astype(bf16), kv[:, 0:C], preferred_element_type=f32) / total
        ms[pl.ds(base, chunk)] = mix.reshape(chunk, per, C).astype(bf16)

        def send(i, c):
            e = base + i

            @pl.when(e != me)
            def _():
                mixed_copy(e).start()
            return c

        lax.fori_loop(0, chunk, send, 0)
        return carry

    lax.fori_loop(0, N // chunk, attend_chunk, 0)
    mr[pl.ds(me, 1)] = ms[pl.ds(me, 1)]

    load_uv.wait()
    weight_arrival(uv_hbm, wv, sv, rv)

    def mixed_arrival(k, carry):
        src = lax.rem(me + k, N)
        rcopy(ms.at[src], mr.at[src], sm.at[src], rm.at[src], lax.div(src, G), lax.rem(src, G)).wait_recv()
        return carry

    lax.fori_loop(1, N, mixed_arrival, 0)
    mixed = mr[...].astype(f32).reshape(expanded, C).astype(bf16)
    values = jnp.dot(mixed, wv[...], preferred_element_type=f32)
    values = jnp.where(own_head, values, 0.0).astype(bf16)
    values = lax.dot_general(pick, values, (((0,), (0,)), ((), ())), preferred_element_type=f32)
    os_[...] = values.reshape(F, steps * G, cols).astype(bf16)

    def out_copy(k):
        t = lax.rem(f + k, F)
        return rcopy(os_.at[t], or_.at[f], so.at[k], ro.at[f], t, hd)

    each(1, F, out_copy, "start")
    or_[pl.ds(f, 1)] = os_[pl.ds(f, 1)]

    def out_arrival(k, carry):
        src = lax.rem(f + k, F)
        rcopy(os_.at[src], or_.at[src], so.at[k], ro.at[src], src, hd).wait_recv()
        return carry

    lax.fori_loop(1, F, out_arrival, 0)
    for p in range(F):
        v = or_[p].astype(f32)
        for s in range(steps):
            out_ref[s, :, p * cols:(p + 1) * cols] = v[s * G:(s + 1) * G].astype(bf16)

    each(1, F, probe_copy, "wait_send")
    each(1, F, uk_copy, "wait_send")
    each(1, F, uv_copy, "wait_send")
    each(1, Z + 1, pair_copy, "wait_send")
    each(1, Z, line_copy, "wait_send")
    each(1, N, query_copy, "wait_send")
    each(1, F, out_copy, "wait_send")

    def mixed_sent(k, carry):
        mixed_copy(lax.rem(me + k, N)).wait_send()
        return carry

    lax.fori_loop(1, N, mixed_sent, 0)


def one_kernel(probe_compressed, w_uq, w_qr, w_uk, w_uv, cache, new_kv, lengths):
    F, G = lax.axis_size("fsdp"), lax.axis_size("head")
    N, Z = F * G, F // 2
    steps, group, _ = probe_compressed.shape
    ck, heads = w_uk.shape[0], w_uk.shape[1] // NOPE
    own = heads // F
    C = ck * F
    queries = F * steps * G
    per = steps * own
    cols, rcols = own * NOPE, own * R
    stored, width = cache.shape[1:]
    half = R // 2
    freqs = 10000.0 ** (-(np.arange(half, dtype=np.float32) * 2.0 / R))
    freqs = np.concatenate([freqs, freqs, np.zeros(128 - R)]).astype(np.float32)[None]
    bf16 = jnp.bfloat16
    vm = lambda *shape: pltpu.VMEM(shape, bf16)
    dma = lambda n: pltpu.SemaphoreType.DMA((n,))
    vmem = pl.BlockSpec(memory_space=pltpu.VMEM)
    hbm = pl.BlockSpec(memory_space=pl.ANY)
    return pl.pallas_call(
        functools.partial(fused, F, G, steps, own),
        out_shape=jax.ShapeDtypeStruct((steps, group, heads * VDIM), bf16),
        in_specs=[pl.BlockSpec(memory_space=pltpu.SMEM), vmem, vmem, vmem, hbm, hbm, hbm, hbm, hbm],
        out_specs=vmem,
        scratch_shapes=[
            vm(*w_uq.shape), vm(*w_qr.shape), vm(C, cols), vm(C, cols), vm(stored + 128, width),
            vm(F, steps * G, w_uq.shape[0]), vm(F, steps * G, w_uq.shape[0]),
            vm(Z, queries, cols + rcols), vm(Z, queries, cols + rcols),
            vm(Z, queries, cols + rcols), vm(Z, queries, cols + rcols),
            vm(N, per, C + 128), vm(N, per, C + 128), vm(N, per, C), vm(N, per, C),
            vm(F, steps * G, cols), vm(F, steps * G, cols),
            dma(5), dma(F), dma(F), dma(F), dma(F), dma(F), dma(F), dma(Z), dma(Z), dma(Z), dma(Z),
            dma(N), dma(N), dma(N), dma(N), dma(F), dma(F),
        ],
        compiler_params=pltpu.CompilerParams(
            collective_id=0, has_side_effects=True, vmem_limit_bytes=48 * 2**20
        ),
    )(lengths, jnp.asarray(freqs), probe_compressed, new_kv, w_uq, w_qr, w_uk, w_uv, cache)


def choose(*arrays):
    probe, w_uk, cache = arrays[0], arrays[3], arrays[5]
    F, G = lax.axis_size("fsdp"), lax.axis_size("head")
    own = w_uk.shape[1] // NOPE // F
    fits = own > 0 and w_uk.shape[1] == own * NOPE * F and F % 2 == 0
    fits = fits and probe.shape[1] == G and cache.shape[0] == 1
    fits = fits and (probe.shape[0] * own) % 8 == 0 and (probe.shape[0] * G) % 8 == 0
    fits = fits and w_uk.shape[0] % 16 == 0 and (own * R) % 128 == 0
    return one_kernel(*arrays) if fits else per_device(*arrays)


def solution(mesh):
    in_specs = (
        P(None, "fsdp", None),
        P("fsdp", "head"),
        P("fsdp", "head"),
        P("fsdp", "head"),
        P("fsdp", "head"),
        P(("fsdp", "head"), None, None),
        P(None, ("fsdp", "head"), None),
        P(("fsdp", "head")),
    )
    out_specs = P(None, "fsdp", "head")
    return jax.shard_map(
        choose, mesh=mesh, in_specs=in_specs, out_specs=out_specs, check_vma=False
    )
```

```python
import functools

import jax
import jax.numpy as jnp
import numpy as np
from jax import lax
from jax.experimental import pallas as pl
from jax.experimental.pallas import tpu as pltpu
from jax.sharding import PartitionSpec as P

NOPE = 128
R = 64
VDIM = 128


def rotate(rope_part, position):
    half = rope_part.shape[-1] // 2
    freqs = 10000.0 ** (-(jnp.arange(half, dtype=jnp.float32) * 2.0 / (2 * half)))
    angle = position[..., None] * freqs
    first = rope_part[..., :half]
    second = rope_part[..., half:]
    cosine_table = jnp.cos(angle)
    sine = jnp.sin(angle)
    return jnp.concatenate(
        [first * cosine_table - second * sine, first * sine + second * cosine_table], axis=-1
    )


def attend(query, keys, fresh, extent):
    steps = query.shape[0]
    heads = query.shape[1]
    width = keys.shape[1]
    latent_width = width - R
    position = (extent + jnp.arange(steps, dtype=jnp.int32)).astype(jnp.float32)
    rotated = rotate(query[:, :, latent_width:].astype(jnp.float32), position[:, None])
    joined = jnp.concatenate([query[:, :, :latent_width], rotated.astype(jnp.bfloat16)], axis=2)
    joined = joined.reshape(steps * heads, width)
    factor = (NOPE + R) ** (-0.5)
    older = jnp.dot(joined, keys.T, preferred_element_type=jnp.float32) * factor
    valid = jnp.arange(keys.shape[0], dtype=jnp.int32) < extent
    older = jnp.where(valid[None, :], older, -1e30)
    newer = jnp.dot(joined, fresh.T, preferred_element_type=jnp.float32) * factor
    order = jnp.arange(steps, dtype=jnp.int32)
    allowed = jnp.repeat(order[None, :] <= order[:, None], heads, axis=0)
    newer = jnp.where(allowed, newer, -1e30)
    highest = jnp.maximum(jnp.max(older, axis=1), jnp.max(newer, axis=1))
    weight_old = jnp.exp(older - highest[:, None])
    weight_new = jnp.exp(newer - highest[:, None])
    total = jnp.sum(weight_old, axis=1) + jnp.sum(weight_new, axis=1)
    mixed = jnp.dot(
        weight_old.astype(jnp.bfloat16), keys[:, :latent_width], preferred_element_type=jnp.float32
    )
    mixed = mixed + jnp.dot(
        weight_new.astype(jnp.bfloat16), fresh[:, :latent_width], preferred_element_type=jnp.float32
    )
    return (mixed / total[:, None]).astype(jnp.bfloat16).reshape(steps, heads, latent_width)


def per_device(probe_compressed, w_uq, w_qr, w_uk, w_uv, cache, new_kv, lengths):
    heads = w_uk.shape[1] // NOPE
    steps, group, rank = probe_compressed.shape
    flattened = probe_compressed.reshape(steps * group, rank)
    key_up, value_up, rotary_up_weight = (
        lax.all_gather(w_uk, "fsdp", axis=0, tiled=True),
        lax.all_gather(w_uv, "fsdp", axis=0, tiled=True),
        lax.all_gather(w_qr, "fsdp", axis=0, tiled=True),
    )
    key_heads = key_up.reshape(key_up.shape[0], heads, NOPE)
    slab = lax.all_gather(w_uq, "fsdp", axis=0, tiled=True)
    count = slab.shape[0]
    slab_heads = slab.reshape(count, heads, NOPE)
    absorbed = jnp.einsum("rhn,chn->hrc", slab_heads, key_heads, preferred_element_type=jnp.float32)
    absorbed = absorbed.astype(jnp.bfloat16)
    summed = jnp.einsum("qr,hrc->qhc", flattened, absorbed, preferred_element_type=jnp.float32)
    latent = summed.astype(jnp.bfloat16)
    latent_rank = key_up.shape[0]
    rope_query = jnp.dot(flattened, rotary_up_weight, preferred_element_type=jnp.float32).astype(
        jnp.bfloat16
    )
    rope_query = rope_query.reshape(steps * group, heads, R)
    query_matrix = jnp.concatenate([latent, rope_query], axis=2).reshape(
        steps, group, heads, latent_rank + R
    )
    row_queries = lax.all_to_all(query_matrix, "head", split_axis=1, concat_axis=2, tiled=True)
    mixed = jax.vmap(attend, in_axes=(1, 0, 1, 0), out_axes=1)(row_queries, cache, new_kv, lengths)
    combined_across_heads = lax.all_to_all(mixed, "head", split_axis=2, concat_axis=1, tiled=True)
    value_heads = value_up.reshape(latent_rank, heads, VDIM)
    attention_output = jnp.einsum(
        "sghc,chv->sghv", combined_across_heads, value_heads, preferred_element_type=jnp.float32
    )
    return attention_output.astype(jnp.bfloat16).reshape(steps, group, heads * VDIM)


def fused(F, G, steps, own,
          len_ref, freq_hbm, probe_hbm, new_hbm, uq_hbm, qr_hbm, uk_hbm, uv_hbm, cache_hbm,
          out_ref,
          freq_ref, probe_ref, new_ref,
          uq, wqr, wk, wv, kv, ps, pr, pp, pv, zs, zr, nq, es_, er_, qs, qr, ms, mr, vs, vr,
          lsem, sp, rp, sk, rk, spp, rpp, sz, rz, sn, rn, se, re_, sq, rq, sm, rm, so, ro):
    f32, bf16 = jnp.float32, jnp.bfloat16
    f = lax.axis_index("fsdp")
    hd = lax.axis_index("head")
    N = F * G
    Z = F // 2
    me = f * G + hd
    z, core = lax.div(f, 2), lax.rem(f, 2)
    ck = uk_hbm.shape[0]
    cols = own * NOPE
    rcols = own * R
    C = ck * F
    stored = cache_hbm.shape[2]
    slice_rank = uq.shape[0]
    per = steps * own
    queries = F * steps * G
    expanded = N * per

    def rcopy(src, dst, ssem, rsem, ff, hh):
        return pltpu.make_async_remote_copy(
            src_ref=src, dst_ref=dst, send_sem=ssem, recv_sem=rsem,
            device_id={"fsdp": ff, "head": hh}, device_id_type=pl.DeviceIdType.MESH,
        )

    def block(t, width):
        return pl.ds(pl.multiple_of(t * width, 128), width)

    hcols = Z * cols
    mine = pl.ds(pl.multiple_of(core * ck, 16), ck)
    load_uq = pltpu.make_async_copy(uq_hbm, uq, lsem.at[0])
    load_qr = pltpu.make_async_copy(qr_hbm, wqr, lsem.at[1])
    load_kv = pltpu.make_async_copy(cache_hbm.at[0], kv, lsem.at[2])
    load_uk = pltpu.make_async_copy(uk_hbm.at[:, block(core, hcols)], wk.at[mine], lsem.at[3])
    load_uv = pltpu.make_async_copy(uv_hbm.at[:, block(core, hcols)], wv.at[mine], lsem.at[4])
    load_probe = pltpu.make_async_copy(probe_hbm, probe_ref, lsem.at[5])
    load_new = pltpu.make_async_copy(new_hbm, new_ref, lsem.at[6])
    load_freq = pltpu.make_async_copy(freq_hbm, freq_ref, lsem.at[7])
    loads = [load_probe, load_uq, load_qr, load_new, load_freq, load_uk, load_kv, load_uv]
    for c in loads:
        c.start()

    bar = pltpu.get_barrier_semaphore()

    def greet(k, carry):
        t = lax.rem(me + k, N)
        pl.semaphore_signal(
            bar, inc=1, device_id={"fsdp": lax.div(t, G), "head": lax.rem(t, G)},
            device_id_type=pl.DeviceIdType.MESH,
        )
        return carry

    lax.fori_loop(1, N, greet, 0)

    load_probe.wait()
    probe8 = jnp.concatenate([probe_ref[s].astype(f32) for s in range(steps)], axis=0)
    for p in range(F):
        ps[p] = probe8[:, p * slice_rank:(p + 1) * slice_rank].astype(bf16)
    pr[pl.ds(f, 1)] = ps[pl.ds(f, 1)]

    pl.semaphore_wait(bar, N - 1)

    def probe_copy(k):
        t = lax.rem(f + k, F)
        return rcopy(ps.at[t], pr.at[f], sp.at[k], rp.at[f], t, hd)

    def weight_copy(i):
        hbm, w = ((uk_hbm, wk), (uv_hbm, wv))[i]
        return rcopy(hbm.at[:, block(1 - core, hcols)], w.at[mine], sk.at[i], rk.at[i], z * 2 + 1 - core, hd)

    def each(first, last, make, method):
        def step(k, carry):
            getattr(make(k), method)()
            return carry
        lax.fori_loop(first, last, step, 0)

    each(1, F, probe_copy, "start")
    weight_copy(0).start()
    weight_copy(1).start()

    load_new.wait()
    load_freq.wait()
    at = lax.broadcasted_iota(jnp.int32, (128, C + R), 0)
    fill = jnp.zeros((128, C + R), f32)
    for s in range(steps):
        fill = jnp.where(at == s, new_ref[0, s:s + 1].astype(f32), fill)
    fresh = fill.astype(bf16)

    row8 = lax.broadcasted_iota(jnp.int32, (per, 128), 0)
    step8 = lax.div(row8, own)
    angle = (len_ref[0] + step8).astype(f32) * freq_ref[...]
    cos8, sin8 = jnp.cos(angle), jnp.sin(angle)

    load_uq.wait()
    load_qr.wait()

    def probe_arrival(k, carry):
        src = lax.rem(f + k, F)
        rcopy(ps.at[src], pr.at[src], sp.at[k], rp.at[src], src, hd).wait_recv()
        return carry

    lax.fori_loop(1, F, probe_arrival, 0)
    probes = pr[...].astype(f32).reshape(queries, slice_rank).astype(bf16)

    def partial_of(t):
        a = jnp.dot(probes, uq[:, block(t, cols)], preferred_element_type=f32)
        b = jnp.dot(probes, wqr[:, block(t, rcols)], preferred_element_type=f32)
        return a, b

    def pair_copy(k):
        zz = lax.rem(z + k, Z)
        return rcopy(pp.at[zz], pv.at[zz], spp.at[zz], rpp.at[zz], z * 2 + 1 - core, hd)

    def to_partner(k, carry):
        zz = lax.rem(z + k, Z)
        a, b = partial_of((1 - core) * Z + zz)
        pp[zz, :, 0:cols] = a.astype(bf16)
        pp[zz, :, cols:cols + rcols] = b.astype(bf16)
        pair_copy(k).start()
        return carry

    lax.fori_loop(1, Z + 1, to_partner, 0)

    def line_copy(k):
        zz = lax.rem(z + k, Z)
        return rcopy(zs.at[zz], zr.at[z], sz.at[zz], rz.at[z], zz * 2 + core, hd)

    def along_line(k, carry):
        zz = lax.rem(z + k, Z)
        a, b = partial_of(core * Z + zz)
        pair_copy(k).wait_recv()
        zs[zz, :, 0:cols] = (a + pv[zz, :, 0:cols].astype(f32)).astype(bf16)
        zs[zz, :, cols:cols + rcols] = (b + pv[zz, :, cols:cols + rcols].astype(f32)).astype(bf16)
        line_copy(k).start()
        return carry

    lax.fori_loop(1, Z, along_line, 0)
    a, b = partial_of(core * Z + z)
    pair_copy(0).wait_recv()
    nope = a + pv[z, :, 0:cols].astype(f32)
    rope = b + pv[z, :, cols:cols + rcols].astype(f32)
    for k in range(1, Z):
        src = lax.rem(z + k, Z)
        rcopy(zs.at[src], zr.at[src], sz.at[src], rz.at[src], src * 2 + core, hd).wait_recv()
        nope = nope + zr[src, :, 0:cols].astype(f32)
        rope = rope + zr[src, :, cols:cols + rcols].astype(f32)
    nq[pl.ds(z, 1)] = nope.astype(bf16).reshape(1, queries, cols)
    rope = rope.astype(bf16)

    def nope_copy(k):
        zz = lax.rem(z + k, Z)
        return rcopy(nq.at[z], nq.at[z], sn.at[k], rn.at[z], zz * 2 + core, hd)

    each(1, Z, nope_copy, "start")

    def iota(shape, axis):
        return lax.broadcasted_iota(jnp.int32, shape, axis)

    er = iota((expanded, queries), 0)
    ed = lax.div(er, per)
    es = lax.div(lax.rem(er, per), own)
    pick = (lax.div(ed, G) * (steps * G) + es * G + lax.rem(ed, G)) == iota((expanded, queries), 1)
    pick = jnp.where(pick, 1.0, 0.0).astype(bf16)
    head_of_row = lax.rem(iota((expanded, cols), 0), own)
    own_head = lax.div(iota((expanded, cols), 1), NOPE) == head_of_row
    own_rope = lax.div(iota((expanded, rcols), 1), R) == lax.rem(iota((expanded, rcols), 0), own)
    fold = lax.rem(iota((rcols, 128), 0), R) == iota((rcols, 128), 1)
    fold = jnp.where(fold, 1.0, 0.0).astype(bf16)
    wide_rope = jnp.where(own_rope, jnp.dot(pick, rope, preferred_element_type=f32), 0.0).astype(bf16)
    rope_rows = jnp.dot(wide_rope, fold, preferred_element_type=f32)
    es_[...] = rope_rows.reshape(N, per, 128).astype(bf16)
    part = hd * 2 + core
    slot = part * Z + z

    def rope_copy(k):
        t = lax.rem(me + k, N)
        return rcopy(es_.at[t], er_.at[slot], se.at[k], re_.at[slot], lax.div(t, G), lax.rem(t, G))

    each(1, N, rope_copy, "start")
    er_[pl.ds(slot, 1)] = es_[pl.ds(me, 1)]

    load_uk.wait()
    theirs = pl.ds(pl.multiple_of((1 - core) * ck, 16), ck)

    def weight_arrival(i):
        hbm, w = ((uk_hbm, wk), (uv_hbm, wv))[i]
        rcopy(hbm.at[:, block(core, hcols)], w.at[theirs], sk.at[i], rk.at[i], z * 2 + 1 - core, hd).wait_recv()

    weight_arrival(0)
    for k in range(1, Z):
        src = lax.rem(z + k, Z)
        rcopy(nq.at[src], nq.at[src], sn.at[k], rn.at[src], src * 2 + core, hd).wait_recv()
    for h in range(Z):
        wide = jnp.where(own_head, jnp.dot(pick, nq[h], preferred_element_type=f32), 0.0).astype(bf16)
        latent = lax.dot_general(
            wide, wk[:, h * cols:(h + 1) * cols], (((1,), (1,)), ((), ())), preferred_element_type=f32
        )
        qs[:, h * per:(h + 1) * per, :] = latent.reshape(N, per, 2 * ck).astype(bf16)

    tall = Z * per

    def tile(p, zz):
        return (pl.ds(pl.multiple_of(p * tall, 16), tall), pl.ds(pl.multiple_of(zz * 2 * ck, 128), 2 * ck))

    def query_copy(k):
        t = lax.rem(me + k, N)
        return rcopy(qs.at[t], qr.at[tile(part, z)], sq.at[k], rq.at[slot], lax.div(t, G), lax.rem(t, G))

    each(1, N, query_copy, "start")
    qr[tile(part, z)] = qs[pl.ds(me, 1)].reshape(tall, 2 * ck)

    load_kv.wait()
    factor = (NOPE + R) ** -0.5
    chunk = F
    keys = stored + 128
    sr = iota((128, 128), 0)
    sc = iota((128, 128), 1)
    half = R // 2
    swap = jnp.where((sr == sc + half) & (sc < half), -1.0, 0.0)
    swap = swap + jnp.where((sr == sc - half) & (sc >= half) & (sc < R), 1.0, 0.0)
    swap = swap.astype(bf16)
    rows = chunk * per
    cosines = jnp.broadcast_to(cos8[None], (chunk, per, 128)).reshape(rows, 128)
    sines = jnp.broadcast_to(sin8[None], (chunk, per, 128)).reshape(rows, 128)
    column = iota((rows, keys), 1)
    step_of = lax.div(lax.rem(iota((rows, keys), 0), per), own)
    shown = (column < len_ref[0]) | ((column >= stored) & (column <= stored + step_of))

    def mixed_copy(b, i):
        zz, cc = lax.div(i, 2), lax.rem(i, 2)
        e = i * G + b
        return rcopy(ms.at[tile(b * 2 + cc, zz)], mr.at[me], sm.at[e], rm.at[me], i, b)

    def attend_chunk(b, carry):
        def arrival(i, c):
            zz, cc = lax.div(i, 2), lax.rem(i, 2)
            at_slot = (b * 2 + cc) * Z + zz

            @pl.when(i * G + b != me)
            def _():
                rcopy(es_.at[0], er_.at[at_slot], se.at[0], re_.at[at_slot], i, b).wait_recv()
                rcopy(qs.at[0], qr.at[tile(b * 2 + cc, zz)], sq.at[0], rq.at[at_slot], i, b).wait_recv()
            return c

        lax.fori_loop(0, chunk, arrival, 0)
        here = pl.ds(pl.multiple_of(b * rows, 16), rows)
        lat = qr[here, :]
        xr = er_[pl.ds(b * chunk, chunk)].astype(f32).reshape(rows, 128)
        turned = jnp.dot(xr.astype(bf16), swap, preferred_element_type=f32)
        rot = (xr * cosines + turned * sines).astype(bf16)[:, 0:R]
        nt = (((1,), (1,)), ((), ()))
        s = jnp.dot(lat, kv[0:C, :], preferred_element_type=f32)
        s = s + jnp.dot(rot, kv[C:C + R, :], preferred_element_type=f32)
        n = lax.dot_general(lat, fresh[:, 0:C], nt, preferred_element_type=f32)
        n = n + lax.dot_general(rot, fresh[:, C:C + R], nt, preferred_element_type=f32)
        s = jnp.concatenate([s, n], axis=1)
        s = jnp.where(shown, s * factor, -1e30)
        m = jnp.max(s, axis=1, keepdims=True)
        w = jnp.exp(s - m)
        total = jnp.sum(w, axis=1, keepdims=True)
        w = w.astype(bf16)
        mix = lax.dot_general(w[:, 0:stored], kv[0:C, :], nt, preferred_element_type=f32)
        mix = mix + jnp.dot(w[:, stored:], fresh[:, 0:C], preferred_element_type=f32)
        ms[here, :] = (mix / total).astype(bf16)

        def send(i, c):
            @pl.when(i * G + b != me)
            def _():
                mixed_copy(b, i).start()
            return c

        lax.fori_loop(0, chunk, send, 0)
        return carry

    lax.fori_loop(0, G, attend_chunk, 0)
    mr[pl.ds(me, 1)] = ms[tile(part, z)].reshape(1, tall, 2 * ck)

    load_uv.wait()
    weight_arrival(1)

    def mixed_arrival(k, carry):
        src = lax.rem(me + k, N)
        rcopy(ms.at[tile(0, 0)], mr.at[src], sm.at[src], rm.at[src], lax.div(src, G), lax.rem(src, G)).wait_recv()
        return carry

    lax.fori_loop(1, N, mixed_arrival, 0)
    for h in range(Z):
        mixed = mr[:, h * per:(h + 1) * per, :].astype(f32).reshape(expanded, 2 * ck).astype(bf16)
        values = jnp.dot(mixed, wv[:, h * cols:(h + 1) * cols], preferred_element_type=f32)
        values = jnp.where(own_head, values, 0.0).astype(bf16)
        values = lax.dot_general(pick, values, (((0,), (0,)), ((), ())), preferred_element_type=f32)
        vs[:, :, h * cols:(h + 1) * cols] = values.reshape(F, steps * G, cols).astype(bf16)

    def out_copy(k):
        t = lax.rem(f + k, F)
        return rcopy(vs.at[t], vr.at[f], so.at[k], ro.at[f], t, hd)

    each(1, F, out_copy, "start")
    vr[pl.ds(f, 1)] = vs[pl.ds(f, 1)]

    def out_arrival(k, carry):
        src = lax.rem(f + k, F)
        rcopy(vs.at[src], vr.at[src], so.at[k], ro.at[src], src, hd).wait_recv()
        return carry

    lax.fori_loop(1, F, out_arrival, 0)
    for p in range(2):
        v = sum(vr[zz * 2 + p].astype(f32) for zz in range(Z))
        for s in range(steps):
            out_ref[s, :, p * hcols:(p + 1) * hcols] = v[s * G:(s + 1) * G].astype(bf16)

    each(1, F, probe_copy, "wait_send")
    weight_copy(0).wait_send()
    weight_copy(1).wait_send()
    each(1, Z, nope_copy, "wait_send")
    each(1, N, rope_copy, "wait_send")
    each(1, Z + 1, pair_copy, "wait_send")
    each(1, Z, line_copy, "wait_send")
    each(1, N, query_copy, "wait_send")
    each(1, F, out_copy, "wait_send")

    def mixed_sent(k, carry):
        t = lax.rem(me + k, N)
        mixed_copy(lax.rem(t, G), lax.div(t, G)).wait_send()
        return carry

    lax.fori_loop(1, N, mixed_sent, 0)


def one_kernel(probe_compressed, w_uq, w_qr, w_uk, w_uv, cache, new_kv, lengths):
    F, G = lax.axis_size("fsdp"), lax.axis_size("head")
    N, Z = F * G, F // 2
    steps, group, _ = probe_compressed.shape
    ck, heads = w_uk.shape[0], w_uk.shape[1] // NOPE
    own = heads // F
    C = ck * F
    queries = F * steps * G
    per = steps * own
    cols, rcols = own * NOPE, own * R
    hcols = Z * cols
    cache = cache.transpose(0, 2, 1)
    new_kv = new_kv.transpose(1, 0, 2)
    half = R // 2
    freqs = 10000.0 ** (-(np.arange(half, dtype=np.float32) * 2.0 / R))
    freqs = np.concatenate([freqs, freqs, np.zeros(128 - R)]).astype(np.float32)[None]
    bf16 = jnp.bfloat16
    vm = lambda *shape: pltpu.VMEM(shape, bf16)
    dma = lambda n: pltpu.SemaphoreType.DMA((n,))
    vmem = pl.BlockSpec(memory_space=pltpu.VMEM)
    hbm = pl.BlockSpec(memory_space=pltpu.HBM)
    return pl.pallas_call(
        functools.partial(fused, F, G, steps, own),
        out_shape=jax.ShapeDtypeStruct((steps, group, heads * VDIM), bf16),
        in_specs=[pl.BlockSpec(memory_space=pltpu.SMEM)] + [hbm] * 8,
        out_specs=vmem,
        scratch_shapes=[
            pltpu.VMEM((1, 128), jnp.float32), vm(*probe_compressed.shape), vm(*new_kv.shape),
            vm(*w_uq.shape), vm(*w_qr.shape), vm(2 * ck, hcols), vm(2 * ck, hcols), vm(*cache.shape[1:]),
            vm(F, steps * G, w_uq.shape[0]), vm(F, steps * G, w_uq.shape[0]),
            vm(Z, queries, cols + rcols), vm(Z, queries, cols + rcols),
            vm(Z, queries, cols + rcols), vm(Z, queries, cols + rcols),
            vm(Z, queries, cols), vm(N, per, 128), vm(N, per, 128),
            vm(N, Z * per, 2 * ck), vm(2 * G * Z * per, C), vm(2 * G * Z * per, C), vm(N, Z * per, 2 * ck),
            vm(F, steps * G, hcols), vm(F, steps * G, hcols),
            dma(8), dma(F), dma(F), dma(2), dma(2), dma(Z), dma(Z), dma(Z), dma(Z), dma(Z), dma(Z),
            dma(N), dma(N), dma(N), dma(N), dma(N), dma(N), dma(F), dma(F),
        ],
        compiler_params=pltpu.CompilerParams(
            collective_id=0, has_side_effects=True, vmem_limit_bytes=48 * 2**20
        ),
    )(lengths, jnp.asarray(freqs), probe_compressed, new_kv, w_uq, w_qr, w_uk, w_uv, cache)


def choose(*arrays):
    probe, w_uk, cache = arrays[0], arrays[3], arrays[5]
    F, G = lax.axis_size("fsdp"), lax.axis_size("head")
    own = w_uk.shape[1] // NOPE // F
    fits = own > 0 and w_uk.shape[1] == own * NOPE * F and F % 2 == 0
    fits = fits and probe.shape[1] == G and cache.shape[0] == 1
    fits = fits and (probe.shape[0] * own) % 8 == 0 and (probe.shape[0] * G) % 8 == 0
    fits = fits and w_uk.shape[0] % 16 == 0 and (2 * w_uk.shape[0]) % 128 == 0 and cache.shape[1] % 128 == 0 and (own * R) % 128 == 0
    return one_kernel(*arrays) if fits else per_device(*arrays)


def solution(mesh):
    in_specs = (
        P(None, "fsdp", None),
        P("fsdp", "head"),
        P("fsdp", "head"),
        P("fsdp", "head"),
        P("fsdp", "head"),
        P(("fsdp", "head"), None, None),
        P(None, ("fsdp", "head"), None),
        P(("fsdp", "head")),
    )
    out_specs = P(None, "fsdp", "head")
    return jax.shard_map(
        choose, mesh=mesh, in_specs=in_specs, out_specs=out_specs, check_vma=False
    )
```

```python
import functools

import jax
import jax.numpy as jnp
import numpy as np
from jax import lax
from jax.experimental import pallas as pl
from jax.experimental.pallas import tpu as pltpu
from jax.sharding import PartitionSpec as P

NOPE = 128
R = 64
VDIM = 128


def rotate(rope_part, position):
    half = rope_part.shape[-1] // 2
    freqs = 10000.0 ** (-(jnp.arange(half, dtype=jnp.float32) * 2.0 / (2 * half)))
    angle = position[..., None] * freqs
    first = rope_part[..., :half]
    second = rope_part[..., half:]
    cosine_table = jnp.cos(angle)
    sine = jnp.sin(angle)
    return jnp.concatenate(
        [first * cosine_table - second * sine, first * sine + second * cosine_table], axis=-1
    )


def attend(query, keys, fresh, extent):
    steps = query.shape[0]
    heads = query.shape[1]
    width = keys.shape[1]
    latent_width = width - R
    position = (extent + jnp.arange(steps, dtype=jnp.int32)).astype(jnp.float32)
    rotated = rotate(query[:, :, latent_width:].astype(jnp.float32), position[:, None])
    joined = jnp.concatenate([query[:, :, :latent_width], rotated.astype(jnp.bfloat16)], axis=2)
    joined = joined.reshape(steps * heads, width)
    factor = (NOPE + R) ** (-0.5)
    older = jnp.dot(joined, keys.T, preferred_element_type=jnp.float32) * factor
    valid = jnp.arange(keys.shape[0], dtype=jnp.int32) < extent
    older = jnp.where(valid[None, :], older, -1e30)
    newer = jnp.dot(joined, fresh.T, preferred_element_type=jnp.float32) * factor
    order = jnp.arange(steps, dtype=jnp.int32)
    allowed = jnp.repeat(order[None, :] <= order[:, None], heads, axis=0)
    newer = jnp.where(allowed, newer, -1e30)
    highest = jnp.maximum(jnp.max(older, axis=1), jnp.max(newer, axis=1))
    weight_old = jnp.exp(older - highest[:, None])
    weight_new = jnp.exp(newer - highest[:, None])
    total = jnp.sum(weight_old, axis=1) + jnp.sum(weight_new, axis=1)
    mixed = jnp.dot(
        weight_old.astype(jnp.bfloat16), keys[:, :latent_width], preferred_element_type=jnp.float32
    )
    mixed = mixed + jnp.dot(
        weight_new.astype(jnp.bfloat16), fresh[:, :latent_width], preferred_element_type=jnp.float32
    )
    return (mixed / total[:, None]).astype(jnp.bfloat16).reshape(steps, heads, latent_width)


def per_device(probe_compressed, w_uq, w_qr, w_uk, w_uv, cache, new_kv, lengths):
    heads = w_uk.shape[1] // NOPE
    steps, group, rank = probe_compressed.shape
    flattened = probe_compressed.reshape(steps * group, rank)
    key_up, value_up, rotary_up_weight = (
        lax.all_gather(w_uk, "fsdp", axis=0, tiled=True),
        lax.all_gather(w_uv, "fsdp", axis=0, tiled=True),
        lax.all_gather(w_qr, "fsdp", axis=0, tiled=True),
    )
    key_heads = key_up.reshape(key_up.shape[0], heads, NOPE)
    slab = lax.all_gather(w_uq, "fsdp", axis=0, tiled=True)
    count = slab.shape[0]
    slab_heads = slab.reshape(count, heads, NOPE)
    absorbed = jnp.einsum("rhn,chn->hrc", slab_heads, key_heads, preferred_element_type=jnp.float32)
    absorbed = absorbed.astype(jnp.bfloat16)
    summed = jnp.einsum("qr,hrc->qhc", flattened, absorbed, preferred_element_type=jnp.float32)
    latent = summed.astype(jnp.bfloat16)
    latent_rank = key_up.shape[0]
    rope_query = jnp.dot(flattened, rotary_up_weight, preferred_element_type=jnp.float32).astype(
        jnp.bfloat16
    )
    rope_query = rope_query.reshape(steps * group, heads, R)
    query_matrix = jnp.concatenate([latent, rope_query], axis=2).reshape(
        steps, group, heads, latent_rank + R
    )
    row_queries = lax.all_to_all(query_matrix, "head", split_axis=1, concat_axis=2, tiled=True)
    mixed = jax.vmap(attend, in_axes=(1, 0, 1, 0), out_axes=1)(row_queries, cache, new_kv, lengths)
    combined_across_heads = lax.all_to_all(mixed, "head", split_axis=2, concat_axis=1, tiled=True)
    value_heads = value_up.reshape(latent_rank, heads, VDIM)
    attention_output = jnp.einsum(
        "sghc,chv->sghv", combined_across_heads, value_heads, preferred_element_type=jnp.float32
    )
    return attention_output.astype(jnp.bfloat16).reshape(steps, group, heads * VDIM)


def fused(F, G, steps, own,
          len_ref, freq_hbm, probe_hbm, new_hbm, uq_hbm, qr_hbm, uk_hbm, uv_hbm, cache_hbm,
          out_ref,
          freq_ref, probe_ref, new_ref,
          uq, wqr, wk, wv, kv, ps, pr, pp, pv, zs, zr, nq, es_, er_, qs, qr, ms, mr, vs, vr,
          lsem, sp, rp, sk, rk, spp, rpp, sz, rz, sn, rn, se, re_, sq, rq, sm, rm, so, ro):
    f32, bf16 = jnp.float32, jnp.bfloat16
    f = lax.axis_index("fsdp")
    hd = lax.axis_index("head")
    N = F * G
    Z = F // 2
    me = f * G + hd
    z, core = lax.div(f, 2), lax.rem(f, 2)
    ck = uk_hbm.shape[0]
    cols = own * NOPE
    rcols = own * R
    C = ck * F
    stored = cache_hbm.shape[2]
    slice_rank = uq.shape[0]
    per = steps * own
    queries = F * steps * G
    expanded = N * per

    def rcopy(src, dst, ssem, rsem, ff, hh):
        return pltpu.make_async_remote_copy(
            src_ref=src, dst_ref=dst, send_sem=ssem, recv_sem=rsem,
            device_id={"fsdp": ff, "head": hh}, device_id_type=pl.DeviceIdType.MESH,
        )

    def block(t, width):
        return pl.ds(pl.multiple_of(t * width, 128), width)

    hcols = Z * cols
    mine = pl.ds(pl.multiple_of(core * ck, 16), ck)
    load_uq = pltpu.make_async_copy(uq_hbm, uq, lsem.at[0])
    load_qr = pltpu.make_async_copy(qr_hbm, wqr, lsem.at[1])
    load_kv = pltpu.make_async_copy(cache_hbm.at[0], kv, lsem.at[2])
    load_uk = pltpu.make_async_copy(uk_hbm.at[:, block(core, hcols)], wk.at[mine], lsem.at[3])
    load_uv = pltpu.make_async_copy(uv_hbm.at[:, block(core, hcols)], wv.at[mine], lsem.at[4])
    load_probe = pltpu.make_async_copy(probe_hbm, probe_ref, lsem.at[5])
    load_new = pltpu.make_async_copy(new_hbm, new_ref, lsem.at[6])
    load_freq = pltpu.make_async_copy(freq_hbm, freq_ref, lsem.at[7])
    loads = [load_probe, load_uq, load_qr, load_new, load_freq, load_uk, load_kv, load_uv]
    for c in loads:
        c.start()

    bar = pltpu.get_barrier_semaphore()

    def greet(k, carry):
        t = lax.rem(me + k, N)
        pl.semaphore_signal(
            bar, inc=1, device_id={"fsdp": lax.div(t, G), "head": lax.rem(t, G)},
            device_id_type=pl.DeviceIdType.MESH,
        )
        return carry

    lax.fori_loop(1, N, greet, 0)

    load_probe.wait()
    probe8 = jnp.concatenate([probe_ref[s].astype(f32) for s in range(steps)], axis=0)
    for p in range(F):
        ps[p] = probe8[:, p * slice_rank:(p + 1) * slice_rank].astype(bf16)
    pr[pl.ds(f, 1)] = ps[pl.ds(f, 1)]

    pl.semaphore_wait(bar, N - 1)

    def probe_copy(k):
        t = lax.rem(f + k, F)
        return rcopy(ps.at[t], pr.at[f], sp.at[k], rp.at[f], t, hd)

    def weight_copy(i):
        hbm, w = ((uk_hbm, wk), (uv_hbm, wv))[i]
        return rcopy(hbm.at[:, block(1 - core, hcols)], w.at[mine], sk.at[i], rk.at[i], z * 2 + 1 - core, hd)

    def each(first, last, make, method):
        def step(k, carry):
            getattr(make(k), method)()
            return carry
        lax.fori_loop(first, last, step, 0)

    each(1, F, probe_copy, "start")
    weight_copy(0).start()
    weight_copy(1).start()

    load_new.wait()
    load_freq.wait()
    at = lax.broadcasted_iota(jnp.int32, (128, C + R), 0)
    fill = jnp.zeros((128, C + R), f32)
    for s in range(steps):
        fill = jnp.where(at == s, new_ref[0, s:s + 1].astype(f32), fill)
    fresh = fill.astype(bf16)

    row8 = lax.broadcasted_iota(jnp.int32, (per, 128), 0)
    step8 = lax.div(row8, own)
    angle = (len_ref[0] + step8).astype(f32) * freq_ref[...]
    cos8, sin8 = jnp.cos(angle), jnp.sin(angle)

    load_uq.wait()
    load_qr.wait()

    def probe_arrival(k, carry):
        src = lax.rem(f + k, F)
        rcopy(ps.at[src], pr.at[src], sp.at[k], rp.at[src], src, hd).wait_recv()
        return carry

    lax.fori_loop(1, F, probe_arrival, 0)
    probes = pr[...].astype(f32).reshape(queries, slice_rank).astype(bf16)

    def partial_of(t):
        a = jnp.dot(probes, uq[:, block(t, cols)], preferred_element_type=f32)
        b = jnp.dot(probes, wqr[:, block(t, rcols)], preferred_element_type=f32)
        return a, b

    def pair_copy(k):
        zz = lax.rem(z + k, Z)
        return rcopy(pp.at[zz], pv.at[zz], spp.at[zz], rpp.at[zz], z * 2 + 1 - core, hd)

    def to_partner(k, carry):
        zz = lax.rem(z + k, Z)
        a, b = partial_of((1 - core) * Z + zz)
        pp[zz, :, 0:cols] = a.astype(bf16)
        pp[zz, :, cols:cols + rcols] = b.astype(bf16)
        pair_copy(k).start()
        return carry

    lax.fori_loop(1, Z + 1, to_partner, 0)

    def line_copy(k):
        zz = lax.rem(z + k, Z)
        return rcopy(zs.at[zz], zr.at[z], sz.at[zz], rz.at[z], zz * 2 + core, hd)

    def along_line(k, carry):
        zz = lax.rem(z + k, Z)
        a, b = partial_of(core * Z + zz)
        pair_copy(k).wait_recv()
        zs[zz, :, 0:cols] = (a + pv[zz, :, 0:cols].astype(f32)).astype(bf16)
        zs[zz, :, cols:cols + rcols] = (b + pv[zz, :, cols:cols + rcols].astype(f32)).astype(bf16)
        line_copy(k).start()
        return carry

    lax.fori_loop(1, Z, along_line, 0)
    a, b = partial_of(core * Z + z)
    pair_copy(0).wait_recv()
    nope = a + pv[z, :, 0:cols].astype(f32)
    rope = b + pv[z, :, cols:cols + rcols].astype(f32)
    for k in range(1, Z):
        src = lax.rem(z + k, Z)
        rcopy(zs.at[src], zr.at[src], sz.at[src], rz.at[src], src * 2 + core, hd).wait_recv()
        nope = nope + zr[src, :, 0:cols].astype(f32)
        rope = rope + zr[src, :, cols:cols + rcols].astype(f32)
    nq[pl.ds(z, 1)] = nope.astype(bf16).reshape(1, queries, cols)
    rope = rope.astype(bf16)

    def nope_copy(k):
        zz = lax.rem(z + k, Z)
        return rcopy(nq.at[z], nq.at[z], sn.at[k], rn.at[z], zz * 2 + core, hd)

    each(1, Z, nope_copy, "start")

    def iota(shape, axis):
        return lax.broadcasted_iota(jnp.int32, shape, axis)

    er = iota((expanded, queries), 0)
    ed = lax.div(er, per)
    es = lax.div(lax.rem(er, per), own)
    pick = (lax.div(ed, G) * (steps * G) + es * G + lax.rem(ed, G)) == iota((expanded, queries), 1)
    pick = jnp.where(pick, 1.0, 0.0).astype(bf16)
    head_of_row = lax.rem(iota((expanded, cols), 0), own)
    own_head = lax.div(iota((expanded, cols), 1), NOPE) == head_of_row
    own_rope = lax.div(iota((expanded, rcols), 1), R) == lax.rem(iota((expanded, rcols), 0), own)
    fold = lax.rem(iota((rcols, 128), 0), R) == iota((rcols, 128), 1)
    fold = jnp.where(fold, 1.0, 0.0).astype(bf16)
    wide_rope = jnp.where(own_rope, jnp.dot(pick, rope, preferred_element_type=f32), 0.0).astype(bf16)
    rope_rows = jnp.dot(wide_rope, fold, preferred_element_type=f32)
    es_[...] = rope_rows.reshape(N, per, 128).astype(bf16)
    part = hd * 2 + core
    slot = part * Z + z

    def rope_copy(k):
        t = lax.rem(me + k, N)
        return rcopy(es_.at[t], er_.at[slot], se.at[k], re_.at[slot], lax.div(t, G), lax.rem(t, G))

    each(1, N, rope_copy, "start")
    er_[pl.ds(slot, 1)] = es_[pl.ds(me, 1)]

    load_uk.wait()
    theirs = pl.ds(pl.multiple_of((1 - core) * ck, 16), ck)

    def weight_arrival(i):
        hbm, w = ((uk_hbm, wk), (uv_hbm, wv))[i]
        rcopy(hbm.at[:, block(core, hcols)], w.at[theirs], sk.at[i], rk.at[i], z * 2 + 1 - core, hd).wait_recv()

    weight_arrival(0)
    for k in range(1, Z):
        src = lax.rem(z + k, Z)
        rcopy(nq.at[src], nq.at[src], sn.at[k], rn.at[src], src * 2 + core, hd).wait_recv()
    for h in range(Z):
        wide = jnp.where(own_head, jnp.dot(pick, nq[h], preferred_element_type=f32), 0.0).astype(bf16)
        latent = lax.dot_general(
            wide, wk[:, h * cols:(h + 1) * cols], (((1,), (1,)), ((), ())), preferred_element_type=f32
        )
        qs[:, h * per:(h + 1) * per, :] = latent.reshape(N, per, 2 * ck).astype(bf16)

    tall = Z * per

    def tile(p, zz):
        return (pl.ds(pl.multiple_of(p * tall, 16), tall), pl.ds(pl.multiple_of(zz * 2 * ck, 128), 2 * ck))

    def query_copy(k):
        ff = lax.rem(f + lax.rem(k, F), F)
        hh = lax.rem(hd + lax.div(k, F), G)
        return rcopy(qs.at[ff * G + hh], qr.at[tile(part, z)], sq.at[k], rq.at[slot], ff, hh)

    each(1, N, query_copy, "start")
    qr[tile(part, z)] = qs[pl.ds(me, 1)].reshape(tall, 2 * ck)

    load_kv.wait()
    factor = (NOPE + R) ** -0.5
    chunk = F
    keys = stored + 128
    sr = iota((128, 128), 0)
    sc = iota((128, 128), 1)
    half = R // 2
    swap = jnp.where((sr == sc + half) & (sc < half), -1.0, 0.0)
    swap = swap + jnp.where((sr == sc - half) & (sc >= half) & (sc < R), 1.0, 0.0)
    swap = swap.astype(bf16)
    rows = chunk * per
    cosines = jnp.broadcast_to(cos8[None], (chunk, per, 128)).reshape(rows, 128)
    sines = jnp.broadcast_to(sin8[None], (chunk, per, 128)).reshape(rows, 128)
    column = iota((rows, keys), 1)
    step_of = lax.div(lax.rem(iota((rows, keys), 0), per), own)
    shown = (column < len_ref[0]) | ((column >= stored) & (column <= stored + step_of))

    def mixed_copy(b, i):
        zz, cc = lax.div(i, 2), lax.rem(i, 2)
        e = i * G + b
        return rcopy(ms.at[tile(b * 2 + cc, zz)], mr.at[me], sm.at[e], rm.at[me], i, b)

    def attend_chunk(turn, carry):
        b = lax.rem(hd + G - turn, G)

        def arrival(i, c):
            zz, cc = lax.div(i, 2), lax.rem(i, 2)
            at_slot = (b * 2 + cc) * Z + zz

            @pl.when(i * G + b != me)
            def _():
                rcopy(es_.at[0], er_.at[at_slot], se.at[0], re_.at[at_slot], i, b).wait_recv()
                rcopy(qs.at[0], qr.at[tile(b * 2 + cc, zz)], sq.at[0], rq.at[at_slot], i, b).wait_recv()
            return c

        lax.fori_loop(0, chunk, arrival, 0)
        here = pl.ds(pl.multiple_of(b * rows, 16), rows)
        lat = qr[here, :]
        xr = er_[pl.ds(b * chunk, chunk)].astype(f32).reshape(rows, 128)
        turned = jnp.dot(xr.astype(bf16), swap, preferred_element_type=f32)
        rot = (xr * cosines + turned * sines).astype(bf16)[:, 0:R]
        nt = (((1,), (1,)), ((), ()))
        s = jnp.dot(lat, kv[0:C, :], preferred_element_type=f32)
        s = s + jnp.dot(rot, kv[C:C + R, :], preferred_element_type=f32)
        n = lax.dot_general(lat, fresh[:, 0:C], nt, preferred_element_type=f32)
        n = n + lax.dot_general(rot, fresh[:, C:C + R], nt, preferred_element_type=f32)
        s = jnp.concatenate([s, n], axis=1)
        s = jnp.where(shown, s * factor, -1e30)
        m = jnp.max(s, axis=1, keepdims=True)
        w = jnp.exp(s - m)
        total = jnp.sum(w, axis=1, keepdims=True)
        w = w.astype(bf16)
        mix = lax.dot_general(w[:, 0:stored], kv[0:C, :], nt, preferred_element_type=f32)
        mix = mix + jnp.dot(w[:, stored:], fresh[:, 0:C], preferred_element_type=f32)
        ms[here, :] = (mix / total).astype(bf16)

        def send(i, c):
            @pl.when(i * G + b != me)
            def _():
                mixed_copy(b, i).start()
            return c

        lax.fori_loop(0, chunk, send, 0)
        return carry

    lax.fori_loop(0, G, attend_chunk, 0)
    mr[pl.ds(me, 1)] = ms[tile(part, z)].reshape(1, tall, 2 * ck)

    load_uv.wait()
    weight_arrival(1)

    def mixed_arrival(k, carry):
        src = lax.rem(me + k, N)
        rcopy(ms.at[tile(0, 0)], mr.at[src], sm.at[src], rm.at[src], lax.div(src, G), lax.rem(src, G)).wait_recv()
        return carry

    lax.fori_loop(1, N, mixed_arrival, 0)
    for h in range(Z):
        mixed = mr[:, h * per:(h + 1) * per, :].astype(f32).reshape(expanded, 2 * ck).astype(bf16)
        values = jnp.dot(mixed, wv[:, h * cols:(h + 1) * cols], preferred_element_type=f32)
        values = jnp.where(own_head, values, 0.0).astype(bf16)
        values = lax.dot_general(pick, values, (((0,), (0,)), ((), ())), preferred_element_type=f32)
        vs[:, :, h * cols:(h + 1) * cols] = values.reshape(F, steps * G, cols).astype(bf16)

    def out_copy(k):
        t = lax.rem(f + k, F)
        return rcopy(vs.at[t], vr.at[f], so.at[k], ro.at[f], t, hd)

    each(1, F, out_copy, "start")
    vr[pl.ds(f, 1)] = vs[pl.ds(f, 1)]

    def out_arrival(k, carry):
        src = lax.rem(f + k, F)
        rcopy(vs.at[src], vr.at[src], so.at[k], ro.at[src], src, hd).wait_recv()
        return carry

    lax.fori_loop(1, F, out_arrival, 0)
    for p in range(2):
        v = sum(vr[zz * 2 + p].astype(f32) for zz in range(Z))
        for s in range(steps):
            out_ref[s, :, p * hcols:(p + 1) * hcols] = v[s * G:(s + 1) * G].astype(bf16)

    each(1, F, probe_copy, "wait_send")
    weight_copy(0).wait_send()
    weight_copy(1).wait_send()
    each(1, Z, nope_copy, "wait_send")
    each(1, N, rope_copy, "wait_send")
    each(1, Z + 1, pair_copy, "wait_send")
    each(1, Z, line_copy, "wait_send")
    each(1, N, query_copy, "wait_send")
    each(1, F, out_copy, "wait_send")

    def mixed_sent(k, carry):
        t = lax.rem(me + k, N)
        mixed_copy(lax.rem(t, G), lax.div(t, G)).wait_send()
        return carry

    lax.fori_loop(1, N, mixed_sent, 0)


def one_kernel(probe_compressed, w_uq, w_qr, w_uk, w_uv, cache, new_kv, lengths):
    F, G = lax.axis_size("fsdp"), lax.axis_size("head")
    N, Z = F * G, F // 2
    steps, group, _ = probe_compressed.shape
    ck, heads = w_uk.shape[0], w_uk.shape[1] // NOPE
    own = heads // F
    C = ck * F
    queries = F * steps * G
    per = steps * own
    cols, rcols = own * NOPE, own * R
    hcols = Z * cols
    cache = cache.transpose(0, 2, 1)
    new_kv = new_kv.transpose(1, 0, 2)
    half = R // 2
    freqs = 10000.0 ** (-(np.arange(half, dtype=np.float32) * 2.0 / R))
    freqs = np.concatenate([freqs, freqs, np.zeros(128 - R)]).astype(np.float32)[None]
    bf16 = jnp.bfloat16
    vm = lambda *shape: pltpu.VMEM(shape, bf16)
    dma = lambda n: pltpu.SemaphoreType.DMA((n,))
    vmem = pl.BlockSpec(memory_space=pltpu.VMEM)
    hbm = pl.BlockSpec(memory_space=pltpu.HBM)
    return pl.pallas_call(
        functools.partial(fused, F, G, steps, own),
        out_shape=jax.ShapeDtypeStruct((steps, group, heads * VDIM), bf16),
        in_specs=[pl.BlockSpec(memory_space=pltpu.SMEM)] + [hbm] * 8,
        out_specs=vmem,
        scratch_shapes=[
            pltpu.VMEM((1, 128), jnp.float32), vm(*probe_compressed.shape), vm(*new_kv.shape),
            vm(*w_uq.shape), vm(*w_qr.shape), vm(2 * ck, hcols), vm(2 * ck, hcols), vm(*cache.shape[1:]),
            vm(F, steps * G, w_uq.shape[0]), vm(F, steps * G, w_uq.shape[0]),
            vm(Z, queries, cols + rcols), vm(Z, queries, cols + rcols),
            vm(Z, queries, cols + rcols), vm(Z, queries, cols + rcols),
            vm(Z, queries, cols), vm(N, per, 128), vm(N, per, 128),
            vm(N, Z * per, 2 * ck), vm(2 * G * Z * per, C), vm(2 * G * Z * per, C), vm(N, Z * per, 2 * ck),
            vm(F, steps * G, hcols), vm(F, steps * G, hcols),
            dma(8), dma(F), dma(F), dma(2), dma(2), dma(Z), dma(Z), dma(Z), dma(Z), dma(Z), dma(Z),
            dma(N), dma(N), dma(N), dma(N), dma(N), dma(N), dma(F), dma(F),
        ],
        compiler_params=pltpu.CompilerParams(
            collective_id=0, has_side_effects=True, vmem_limit_bytes=67043328
        ),
    )(lengths, jnp.asarray(freqs), probe_compressed, new_kv, w_uq, w_qr, w_uk, w_uv, cache)


def choose(*arrays):
    probe, w_uk, cache = arrays[0], arrays[3], arrays[5]
    F, G = lax.axis_size("fsdp"), lax.axis_size("head")
    own = w_uk.shape[1] // NOPE // F
    fits = own > 0 and w_uk.shape[1] == own * NOPE * F and F % 2 == 0
    fits = fits and probe.shape[1] == G and cache.shape[0] == 1
    fits = fits and (probe.shape[0] * own) % 8 == 0 and (probe.shape[0] * G) % 8 == 0
    fits = fits and w_uk.shape[0] % 16 == 0 and (2 * w_uk.shape[0]) % 128 == 0 and cache.shape[1] % 128 == 0 and (own * R) % 128 == 0
    return one_kernel(*arrays) if fits else per_device(*arrays)


def solution(mesh):
    in_specs = (
        P(None, "fsdp", None),
        P("fsdp", "head"),
        P("fsdp", "head"),
        P("fsdp", "head"),
        P("fsdp", "head"),
        P(("fsdp", "head"), None, None),
        P(None, ("fsdp", "head"), None),
        P(("fsdp", "head")),
    )
    out_specs = P(None, "fsdp", "head")
    return jax.shard_map(
        choose, mesh=mesh, in_specs=in_specs, out_specs=out_specs, check_vma=False
    )
```
